128 devices in a mesh: row: 8 (over x, y_hi), col: 16 (over z, y_lo, core).
Axes of the slice: x: 4, y: 4 (y_hi: 2, y_lo: 2; y = y_hi * 2 + y_lo), z: 4, core: 2. Of those that a mesh axis runs over, the one named last changes fastest.
Arguments:
- old_residual: float32 [8192, 16384], P(('row', 'col')), may hold values from -6 to 6
- group_map: int32 [128, 8], replicated, may hold values from 0 to 1023, as said below
- q_factor: float32 [16384, 32], P('col', 'row'), may hold values from -0.046875 to 0.046875
Outputs:
- relaid: float32 [8192, 16384], P('row', 'col')
- projection: float32 [32, 8192], P(None, ('row', 'col'))
- row_norms: float32 [8192], P(('row', 'col'))
The draws below stay inside these ranges and needn't reach their ends.
Inputs may be any that keep to these rules, and one draw needn't show every extreme that they name: `group_map`: all entries together are each group id 0 to 1023 once; row d (old device d) holds exactly one id of each range k * 128 to (k + 1) * 128 - 1, in any slot order.
All inputs are finite; a program needn't handle non-finite values.
Results may differ from the reference program's by a relative error of at most 0.00007.
Values sent between devices are 32-bit elements; how exact they have to be, the bound alone decides.
No kernel may reach another device: no remote copies, remote signals or barrier semaphores. Data moves between devices by JAX's collectives and lax.ppermute only.
A program may use at most 64 MiB of HBM per device.

```python
import jax
import jax.numpy as jnp
from jax import lax

D = 16384
RANK = 32
CH = 8
ROWS = 8192
N_ROW = 8
DEVICES = 128


def draw_group_map(key, part):
    first_key = jax.random.fold_in(key, 11)
    second_key = jax.random.fold_in(key, 23)
    block_keys = jax.random.split(first_key, N_ROW)
    permuted = jax.vmap(lambda single: jax.random.permutation(single, DEVICES))(block_keys)
    group_ids = (permuted + jnp.arange(N_ROW, dtype=jnp.int32)[:, None] * DEVICES).T
    slot_keys = jax.random.split(second_key, DEVICES)
    slot_order = jax.vmap(lambda single: jax.random.permutation(single, N_ROW))(slot_keys)
    return jnp.take_along_axis(group_ids, slot_order, axis=1).astype(jnp.int32)


def shard_levels(key, shape, pieces, low, high):
    gain = 1.0
    for position, parts in pieces:
        steps = jax.random.uniform(jax.random.fold_in(jax.random.fold_in(key, 6), position), (parts,), jnp.float32, low / len(pieces), high / len(pieces))
        gain = gain * jnp.repeat(jnp.exp(steps), shape[position] // parts).reshape((-1,) + (1,) * (len(shape) - 1 - position))
    return gain


def normal_values(key, shape, deviation, bound, pieces=(), kind=jnp.bfloat16):
    array = deviation * jax.random.normal(key, shape, jnp.float32)
    if pieces:
        array = array * shard_levels(key, shape, pieces, -0.22, 0.18)
    return jnp.clip(array, -bound, bound).astype(kind)


def setup_inputs(seed: int = 0) -> dict:
    streams_of = jax.random.split(jax.random.key(seed), 4)
    return {
        "old_residual": normal_values(streams_of[0], (ROWS, D), 1.0, 6.0, ((0, 128),), jnp.float32),
        "group_map": draw_group_map(jax.random.fold_in(streams_of[3], 71), 0),
        "q_factor": normal_values(streams_of[2], (D, RANK), D ** -0.5, 0.046875, ((0, 16), (1, 8)), jnp.float32),
    }


epsilon = 1e-06

def reference(old_residual, group_map, q_factor):
    group_ids = group_map.reshape(-1).astype(jnp.int32)
    ordering = jnp.argsort(group_ids).astype(jnp.int32)
    groups = old_residual.reshape(DEVICES * N_ROW, CH, D)
    relaid = jnp.take(groups, ordering, axis=0).reshape(ROWS, D)
    product = jnp.dot(relaid, q_factor, precision=lax.Precision.HIGHEST, preferred_element_type=jnp.float32)
    row_norms = jnp.sqrt(lax.optimization_barrier(jnp.mean(relaid * relaid, axis=1)) + epsilon)
    return (relaid, product.T, row_norms)
```

```python
import jax
import jax.numpy as jnp
from jax import lax
from jax.experimental import pallas as pl
from jax.experimental.pallas import tpu as pltpu
from jax.sharding import Mesh, PartitionSpec as P

epsilon = 1e-06
ROW = ("x", "yh")
COL = ("z", "yl", "core")
ALL = ROW + COL


def order_slots(ids_ref, where_ref, source_ref, out_ref, sems):
    count = source_ref.shape[0]
    copies = []
    for slot in range(count):
        block = ids_ref[slot, where_ref[0]] // where_ref[1]
        copy = pltpu.make_async_copy(source_ref.at[slot], out_ref.at[block], sems.at[slot])
        copy.start()
        copies.append(copy)
    for copy in copies:
        copy.wait()


def place_and_reduce(place_ref, factor_ref, received_ref, relaid_ref, share_ref, data, sums, load_sems, store_sem):
    blocks, per_block, rows, width = data.shape
    rank = factor_ref.shape[0]
    loads = [
        pltpu.make_async_copy(received_ref.at[pl.ds(b * per_block, per_block)], data.at[b], load_sems.at[b])
        for b in range(blocks)
    ]
    for load in loads:
        load.start()
    factor = factor_ref[...]
    factor_high = factor.astype(jnp.bfloat16)
    factor_low = (factor - factor_high.astype(jnp.float32)).astype(jnp.bfloat16)
    filler = jnp.zeros((128 - 2 * rank, width), jnp.bfloat16)
    factors = jnp.concatenate([factor_high, factor_low, filler], axis=0)
    lane = lax.broadcasted_iota(jnp.int32, (per_block * rows, 128), 1)
    for b in range(blocks):
        loads[b].wait()
        for i in range(per_block):
            place = place_ref[b * per_block + i]
            pltpu.make_async_copy(data.at[b, i], relaid_ref.at[place], store_sem).start()
        part = data[b].reshape(per_block * rows, width)
        high = part.astype(jnp.bfloat16)
        low = (part - high.astype(jnp.float32)).astype(jnp.bfloat16)
        over = (((1,), (1,)), ((), ()))
        product = lax.dot_general(high, factors, over, preferred_element_type=jnp.float32)
        product += lax.dot_general(low, factors, over, preferred_element_type=jnp.float32)
        squares = jnp.sum(part * part, axis=1, keepdims=True)
        product = jnp.where(lane == 2 * rank, squares, product)
        for i in range(per_block):
            place = place_ref[b * per_block + i]
            sums[pl.ds(pl.multiple_of(place * rows, rows), rows), :] = product[i * rows : (i + 1) * rows]
    half = rank // 2
    for c in range(0, share_ref.shape[0], 2):
        turned = sums[c * 64 : (c + 2) * 64, :].T
        shares = turned[:rank] + turned[rank : 2 * rank]
        squares = turned[2 * rank : 2 * rank + 8]
        for i in range(2):
            lanes = slice(i * 64, (i + 1) * 64)
            share_ref[c + i, :half, :] = jnp.concatenate([shares[:half, lanes], shares[half:, lanes]], axis=1)
            share_ref[c + i, half:, :] = jnp.concatenate([squares[:, lanes], squares[:, lanes]], axis=1)
    pltpu.make_async_copy(data, data, store_sem).wait()


def finish(shares_ref, projection_ref, norms_ref, *, full_width):
    half = projection_ref.shape[0] // 2
    total = jnp.sum(shares_ref[...], axis=0)
    projection_ref[:half, :] = total[:half, :64]
    projection_ref[half:, :] = total[:half, 64:]
    norms_ref[...] = jnp.sqrt(total[half : half + 1, :64] / full_width + epsilon)


def gathered_factor(shard):
    other = lax.ppermute(shard, "yh", [(0, 1), (1, 0)])
    low = lax.axis_index("yh") == 0
    pair = jnp.stack([jnp.where(low, shard, other), jnp.where(low, other, shard)])
    count = lax.axis_size("x")
    tiles = [pair]
    for step in range(1, count):
        tiles.append(lax.ppermute(pair, "x", [(i, (i - step) % count) for i in range(count)]))
    ring = jnp.roll(jnp.stack(tiles), lax.axis_index("x"), axis=0)
    return ring.reshape(-1, shard.shape[1])


def on_device(old_residual, group_map, q_factor):
    rows_total = lax.axis_size(ROW)
    columns_total = lax.axis_size(COL)
    devices = rows_total * columns_total
    my_row = lax.axis_index(ROW)
    position = lax.axis_index(ALL)
    group_rows = old_residual.shape[0] // rows_total
    full_width = old_residual.shape[1]
    width = full_width // columns_total
    rank = q_factor.shape[1] * rows_total
    own_rows = devices * group_rows // columns_total
    ids = group_map.T.astype(jnp.int32)
    source = old_residual.reshape(rows_total, group_rows, columns_total, width).transpose(0, 2, 1, 3)
    any_space = pl.BlockSpec(memory_space=pl.ANY)
    smem = pl.BlockSpec(memory_space=pltpu.SMEM)
    vmem = pl.BlockSpec(memory_space=pltpu.VMEM)
    pieces = pl.pallas_call(
        order_slots,
        out_shape=jax.ShapeDtypeStruct(source.shape, jnp.float32),
        in_specs=[smem, smem, any_space],
        out_specs=any_space,
        scratch_shapes=[pltpu.SemaphoreType.DMA((rows_total,))],
        name="order_slots",
    )(ids, jnp.stack([position, jnp.int32(devices)]), source)
    pieces = pieces.reshape(devices, group_rows, width)
    received = lax.all_to_all(pieces, ALL, 0, 0, tiled=True)
    factor = gathered_factor(q_factor.T)
    place = jnp.sum(jnp.where(ids // devices == my_row, ids % devices, 0), axis=0)
    blocks = 8
    relaid, shares = pl.pallas_call(
        place_and_reduce,
        out_shape=(
            jax.ShapeDtypeStruct((devices, group_rows, width), jnp.float32),
            jax.ShapeDtypeStruct((columns_total, rank // 2 + 8, 2 * own_rows), jnp.float32),
        ),
        in_specs=[smem, vmem, any_space],
        out_specs=(any_space, vmem),
        scratch_shapes=[
            pltpu.VMEM((blocks, devices // blocks, group_rows, width), jnp.float32),
            pltpu.VMEM((devices * group_rows, 128), jnp.float32),
            pltpu.SemaphoreType.DMA((blocks,)),
            pltpu.SemaphoreType.DMA,
        ],
        name="place_and_reduce",
    )(place, factor, received)
    shares = lax.all_to_all(shares, COL, 0, 0, tiled=True)
    projection, norms = pl.pallas_call(
        lambda *refs: finish(*refs, full_width=full_width),
        out_shape=(
            jax.ShapeDtypeStruct((rank, own_rows), jnp.float32),
            jax.ShapeDtypeStruct((1, own_rows), jnp.float32),
        ),
        in_specs=[vmem],
        out_specs=(vmem, vmem),
        name="finish",
    )(shares)
    return relaid.reshape(devices * group_rows, width), projection, norms.reshape(own_rows)


def solution(mesh):
    parts = Mesh(mesh.devices.reshape(4, 2, 4, 2, 2), ALL)
    return jax.shard_map(
        on_device,
        mesh=parts,
        in_specs=(P(ALL, None), P(), P(COL, ROW)),
        out_specs=(P(ROW, COL), P(None, ALL), P(ALL)),
        check_vma=False,
    )
```

```python
import jax
import jax.numpy as jnp
from jax import lax
from jax.experimental import pallas as pl
from jax.experimental.pallas import tpu as pltpu
from jax.sharding import Mesh, PartitionSpec as P

epsilon = 1e-06
ROW = ("x", "yh")
COL = ("z", "yl", "core")
ALL = ROW + COL


def order_slots(ids_ref, where_ref, source_ref, out_ref, data, load_sems, store_sem):
    count = source_ref.shape[0]
    loads = [pltpu.make_async_copy(source_ref.at[j], data.at[j], load_sems.at[j]) for j in range(count)]
    for load in loads:
        load.start()
    for slot in range(count):
        block = ids_ref[slot, where_ref[0]] // where_ref[1]
        loads[slot].wait()
        pltpu.make_async_copy(data.at[slot], out_ref.at[block], store_sem).start()
    pltpu.make_async_copy(data, out_ref, store_sem).wait()


def place_and_reduce(place_ref, factor_ref, received_ref, relaid_ref, share_ref, data, sums, load_sems, store_sem):
    blocks, per_block, rows, width = data.shape
    rank = factor_ref.shape[0]
    loads = [
        pltpu.make_async_copy(received_ref.at[pl.ds(b * per_block, per_block)], data.at[b], load_sems.at[b])
        for b in range(blocks)
    ]
    for load in loads:
        load.start()
    factor = factor_ref[...]
    factor_high = factor.astype(jnp.bfloat16)
    factor_low = (factor - factor_high.astype(jnp.float32)).astype(jnp.bfloat16)
    filler = jnp.zeros((128 - 2 * rank, width), jnp.bfloat16)
    factors = jnp.concatenate([factor_high, factor_low, filler], axis=0)
    lane = lax.broadcasted_iota(jnp.int32, (per_block * rows, 128), 1)
    for b in range(blocks):
        loads[b].wait()
        for i in range(per_block):
            place = place_ref[b * per_block + i]
            pltpu.make_async_copy(data.at[b, i], relaid_ref.at[place], store_sem).start()
        part = data[b].reshape(per_block * rows, width)
        high = part.astype(jnp.bfloat16)
        low = (part - high.astype(jnp.float32)).astype(jnp.bfloat16)
        over = (((1,), (1,)), ((), ()))
        product = lax.dot_general(high, factors, over, preferred_element_type=jnp.float32)
        product += lax.dot_general(low, factors, over, preferred_element_type=jnp.float32)
        squares = jnp.sum(part * part, axis=1, keepdims=True)
        product = jnp.where(lane == 2 * rank, squares, product)
        for i in range(per_block):
            place = place_ref[b * per_block + i]
            sums[pl.ds(pl.multiple_of(place * rows, rows), rows), :] = product[i * rows : (i + 1) * rows]
    half = rank // 2
    for c in range(0, share_ref.shape[0], 2):
        turned = sums[c * 64 : (c + 2) * 64, :].T
        shares = turned[:rank] + turned[rank : 2 * rank]
        squares = turned[2 * rank : 2 * rank + 8]
        for i in range(2):
            lanes = slice(i * 64, (i + 1) * 64)
            share_ref[c + i, :half, :] = jnp.concatenate([shares[:half, lanes], shares[half:, lanes]], axis=1)
            share_ref[c + i, half:, :] = jnp.concatenate([squares[:, lanes], squares[:, lanes]], axis=1)
    pltpu.make_async_copy(received_ref, relaid_ref, store_sem).wait()


def finish(shares_ref, projection_ref, norms_ref, *, full_width):
    half = projection_ref.shape[0] // 2
    total = jnp.sum(shares_ref[...], axis=0)
    projection_ref[:half, :] = total[:half, :64]
    projection_ref[half:, :] = total[:half, 64:]
    norms_ref[...] = jnp.sqrt(total[half : half + 1, :64] / full_width + epsilon)


def gathered_factor(shard, other):
    low = lax.axis_index("yh") == 0
    pair = jnp.stack([jnp.where(low, shard, other), jnp.where(low, other, shard)])
    count = lax.axis_size("x")
    tiles = [pair]
    for step in range(1, count):
        tiles.append(lax.ppermute(pair, "x", [(i, (i - step) % count) for i in range(count)]))
    ring = jnp.roll(jnp.stack(tiles), lax.axis_index("x"), axis=0)
    return ring.reshape(-1, shard.shape[1])


def on_device(old_residual, group_map, q_factor):
    rows_total = lax.axis_size(ROW)
    columns_total = lax.axis_size(COL)
    devices = rows_total * columns_total
    my_row = lax.axis_index(ROW)
    position = lax.axis_index(ALL)
    group_rows = old_residual.shape[0] // rows_total
    full_width = old_residual.shape[1]
    width = full_width // columns_total
    rank = q_factor.shape[1] * rows_total
    own_rows = devices * group_rows // columns_total
    ids = group_map.T.astype(jnp.int32)
    source = old_residual.reshape(rows_total, group_rows, columns_total, width).transpose(0, 2, 1, 3)
    hbm = pl.BlockSpec(memory_space=pltpu.HBM)
    smem = pl.BlockSpec(memory_space=pltpu.SMEM)
    vmem = pl.BlockSpec(memory_space=pltpu.VMEM)
    shard = q_factor.T
    other = lax.ppermute(shard, "yh", [(0, 1), (1, 0)])
    pieces = pl.pallas_call(
        order_slots,
        out_shape=jax.ShapeDtypeStruct(source.shape, jnp.float32),
        in_specs=[smem, smem, hbm],
        out_specs=hbm,
        scratch_shapes=[
            pltpu.VMEM(source.shape, jnp.float32),
            pltpu.SemaphoreType.DMA((rows_total,)),
            pltpu.SemaphoreType.DMA,
        ],
        name="order_slots",
    )(ids, jnp.stack([position, jnp.int32(devices)]), source)
    pieces, other = lax.optimization_barrier((pieces.reshape(devices, group_rows, width), other))
    received = lax.all_to_all(pieces, ALL, 0, 0, tiled=True)
    factor = gathered_factor(shard, other)
    place = jnp.sum(jnp.where(ids // devices == my_row, ids % devices, 0), axis=0)
    blocks = 8
    relaid, shares = pl.pallas_call(
        place_and_reduce,
        out_shape=(
            jax.ShapeDtypeStruct((devices, group_rows, width), jnp.float32),
            jax.ShapeDtypeStruct((columns_total, rank // 2 + 8, 2 * own_rows), jnp.float32),
        ),
        in_specs=[smem, vmem, hbm],
        out_specs=(hbm, vmem),
        scratch_shapes=[
            pltpu.VMEM((blocks, devices // blocks, group_rows, width), jnp.float32),
            pltpu.VMEM((devices * group_rows, 128), jnp.float32),
            pltpu.SemaphoreType.DMA((blocks,)),
            pltpu.SemaphoreType.DMA,
        ],
        name="place_and_reduce",
    )(place, factor, received)
    shares = lax.all_to_all(shares, COL, 0, 0, tiled=True)
    projection, norms = pl.pallas_call(
        lambda *refs: finish(*refs, full_width=full_width),
        out_shape=(
            jax.ShapeDtypeStruct((rank, own_rows), jnp.float32),
            jax.ShapeDtypeStruct((1, own_rows), jnp.float32),
        ),
        in_specs=[vmem],
        out_specs=(vmem, vmem),
        name="finish",
    )(shares)
    return relaid.reshape(devices * group_rows, width), projection, norms.reshape(own_rows)


def solution(mesh):
    parts = Mesh(mesh.devices.reshape(4, 2, 4, 2, 2), ALL)
    return jax.shard_map(
        on_device,
        mesh=parts,
        in_specs=(P(ALL, None), P(), P(COL, ROW)),
        out_specs=(P(ROW, COL), P(None, ALL), P(ALL)),
        check_vma=False,
    )
```

```python
import jax
import jax.numpy as jnp
from jax import lax
from jax.experimental import pallas as pl
from jax.experimental.pallas import tpu as pltpu
from jax.sharding import Mesh, PartitionSpec as P

epsilon = 1e-06
ROW = ("x", "yh")
COL = ("z", "yl", "core")
ALL = ROW + COL
MIB = 1 << 20


def order_slots(ids_hbm, source_ref, out_ref, data, ids_ref, ids_sem, load_sems, store_sem):
    count = source_ref.shape[0]
    devices = ids_hbm.shape[1]
    ids_copy = pltpu.make_async_copy(ids_hbm, ids_ref, ids_sem)
    ids_copy.start()
    loads = [pltpu.make_async_copy(source_ref.at[j], data.at[j], load_sems.at[j]) for j in range(count)]
    for load in loads:
        load.start()
    position = lax.axis_index(ALL)
    ids_copy.wait()
    for slot in range(count):
        block = ids_ref[slot, position] // devices
        loads[slot].wait()
        pltpu.make_async_copy(data.at[slot], out_ref.at[block], store_sem).start()
    pltpu.make_async_copy(data, out_ref, store_sem).wait()


def reduce_groups(place_hbm, *refs):
    tile_refs, (received_ref, share_ref, data, sums, tiles, place_ref, place_sem, load_sems) = refs[:-8], refs[-8:]
    blocks, per_block, rows, width = data.shape
    loads = [
        pltpu.make_async_copy(received_ref.at[pl.ds(b * per_block, per_block)], data.at[b], load_sems.at[b])
        for b in range(blocks)
    ]
    for load in loads:
        load.start()
    place_copy = pltpu.make_async_copy(place_hbm, place_ref, place_sem)
    place_copy.start()
    count = len(tile_refs)
    my_row = lax.axis_index(ROW)
    for step, tile_ref in enumerate(tile_refs):
        tiles[(my_row - step + count) % count] = tile_ref[...]
    factor = jnp.concatenate([tiles[i] for i in range(count)], axis=0)
    rank = factor.shape[0]
    factor_high = factor.astype(jnp.bfloat16)
    factor_low = (factor - factor_high.astype(jnp.float32)).astype(jnp.bfloat16)
    filler = jnp.zeros((128 - 2 * rank, width), jnp.bfloat16)
    factors = jnp.concatenate([factor_high, factor_low, filler], axis=0)
    lane = lax.broadcasted_iota(jnp.int32, (per_block * rows, 128), 1)
    place_copy.wait()
    for b in range(blocks):
        loads[b].wait()
        part = data[b].reshape(per_block * rows, width)
        high = part.astype(jnp.bfloat16)
        low = (part - high.astype(jnp.float32)).astype(jnp.bfloat16)
        over = (((1,), (1,)), ((), ()))
        product = lax.dot_general(high, factors, over, preferred_element_type=jnp.float32)
        product += lax.dot_general(low, factors, over, preferred_element_type=jnp.float32)
        squares = jnp.sum(part * part, axis=1, keepdims=True)
        product = jnp.where(lane == 2 * rank, squares, product)
        for i in range(per_block):
            place = place_ref[b * per_block + i]
            sums[pl.ds(pl.multiple_of(place * rows, rows), rows), :] = product[i * rows : (i + 1) * rows]
    half = rank // 2
    for c in range(0, share_ref.shape[0], 2):
        turned = sums[c * 64 : (c + 2) * 64, :].T
        shares = turned[:rank] + turned[rank : 2 * rank]
        squares = turned[2 * rank : 2 * rank + 8]
        for i in range(2):
            lanes = slice(i * 64, (i + 1) * 64)
            share_ref[c + i, :half, :] = jnp.concatenate([shares[:half, lanes], shares[half:, lanes]], axis=1)
            share_ref[c + i, half:, :] = jnp.concatenate([squares[:, lanes], squares[:, lanes]], axis=1)


def place_groups(place_hbm, received_ref, relaid_ref, data, place_ref, place_sem, load_sems, store_sem):
    blocks, per_block = data.shape[:2]
    place_copy = pltpu.make_async_copy(place_hbm, place_ref, place_sem)
    place_copy.start()
    loads = [
        pltpu.make_async_copy(received_ref.at[pl.ds(b * per_block, per_block)], data.at[b], load_sems.at[b])
        for b in range(blocks)
    ]
    for load in loads:
        load.start()
    place_copy.wait()
    for b in range(blocks):
        loads[b].wait()
        for i in range(per_block):
            place = place_ref[b * per_block + i]
            pltpu.make_async_copy(data.at[b, i], relaid_ref.at[place], store_sem).start()
    pltpu.make_async_copy(received_ref, relaid_ref, store_sem).wait()


def finish(shares_ref, projection_ref, norms_ref, *, full_width):
    half = projection_ref.shape[0] // 2
    total = jnp.sum(shares_ref[...], axis=0)
    projection_ref[:half, :] = total[:half, :64]
    projection_ref[half:, :] = total[:half, 64:]
    norms_ref[...] = jnp.sqrt(total[half : half + 1, :64] / full_width + epsilon)


def on_device(old_residual, group_map, q_factor):
    rows_total = lax.axis_size(ROW)
    columns_total = lax.axis_size(COL)
    devices = rows_total * columns_total
    group_rows = old_residual.shape[0] // rows_total
    full_width = old_residual.shape[1]
    width = full_width // columns_total
    rank = q_factor.shape[1] * rows_total
    own_rows = devices * group_rows // columns_total
    ids = group_map.T
    source = old_residual.reshape(rows_total, group_rows, columns_total, width).transpose(0, 2, 1, 3)
    hbm = pl.BlockSpec(memory_space=pltpu.HBM)
    vmem = pl.BlockSpec(memory_space=pltpu.VMEM)
    f32 = jnp.float32
    dma = pltpu.SemaphoreType.DMA
    pieces = pl.pallas_call(
        order_slots,
        out_shape=jax.ShapeDtypeStruct(source.shape, f32),
        in_specs=[hbm, hbm],
        out_specs=hbm,
        scratch_shapes=[
            pltpu.VMEM(source.shape, f32),
            pltpu.SMEM(ids.shape, jnp.int32),
            dma,
            dma((rows_total,)),
            dma,
        ],
        name="order_slots",
    )(ids, source)
    pieces = pieces.reshape(devices, group_rows, width)
    received = lax.all_to_all(pieces, ALL, 0, 0, tiled=True)
    tiles = [q_factor.T]
    for step in range(1, rows_total):
        ring = [(i, (i + step) % rows_total) for i in range(rows_total)]
        tiles.append(lax.ppermute(tiles[0], ROW, ring))
    place = jnp.sum(jnp.where(ids // devices == lax.axis_index(ROW), ids % devices, 0), axis=0)
    blocks = 8
    staged = (blocks, devices // blocks, group_rows, width)
    shares = pl.pallas_call(
        reduce_groups,
        out_shape=jax.ShapeDtypeStruct((columns_total, rank // 2 + 8, 2 * own_rows), f32),
        in_specs=[hbm] + [vmem] * rows_total + [hbm],
        out_specs=vmem,
        scratch_shapes=[
            pltpu.VMEM(staged, f32),
            pltpu.VMEM((devices * group_rows, 128), f32),
            pltpu.VMEM((rows_total, rank // rows_total, width), f32),
            pltpu.SMEM((devices,), jnp.int32),
            dma,
            dma((blocks,)),
        ],
        compiler_params=pltpu.CompilerParams(vmem_limit_bytes=16 * MIB),
        name="reduce_groups",
    )(place, *tiles, received)
    relaid = pl.pallas_call(
        place_groups,
        out_shape=jax.ShapeDtypeStruct(received.shape, f32),
        in_specs=[hbm, hbm],
        out_specs=hbm,
        scratch_shapes=[
            pltpu.VMEM(staged, f32),
            pltpu.SMEM((devices,), jnp.int32),
            dma,
            dma((blocks,)),
            dma,
        ],
        name="place_groups",
    )(place, received)
    shares = lax.all_to_all(shares, COL, 0, 0, tiled=True)
    projection, norms = pl.pallas_call(
        lambda *refs: finish(*refs, full_width=full_width),
        out_shape=(
            jax.ShapeDtypeStruct((rank, own_rows), f32),
            jax.ShapeDtypeStruct((1, own_rows), f32),
        ),
        in_specs=[vmem],
        out_specs=(vmem, vmem),
        compiler_params=pltpu.CompilerParams(vmem_limit_bytes=4 * MIB),
        name="finish",
    )(shares)
    return relaid.reshape(devices * group_rows, width), projection, norms.reshape(own_rows)


def solution(mesh):
    parts = Mesh(mesh.devices.reshape(4, 2, 4, 2, 2), ALL)
    return jax.shard_map(
        on_device,
        mesh=parts,
        in_specs=(P(ALL, None), P(), P(COL, ROW)),
        out_specs=(P(ROW, COL), P(None, ALL), P(ALL)),
        check_vma=False,
    )
```

```python
import jax
import jax.numpy as jnp
from jax import lax
from jax.experimental import pallas as pl
from jax.experimental.pallas import tpu as pltpu
from jax.sharding import Mesh, PartitionSpec as P

epsilon = 1e-06
ROW = ("x", "yh")
COL = ("z", "yl", "core")
ALL = ROW + COL
MIB = 1 << 20


def order_slots(ids_hbm, source_ref, out_ref, data, ids_ref, ids_sem, load_sems, store_sem):
    count = source_ref.shape[0]
    devices = ids_hbm.shape[1]
    ids_copy = pltpu.make_async_copy(ids_hbm, ids_ref, ids_sem)
    ids_copy.start()
    loads = [pltpu.make_async_copy(source_ref.at[j], data.at[j], load_sems.at[j]) for j in range(count)]
    for load in loads:
        load.start()
    position = lax.axis_index(ALL)
    ids_copy.wait()
    for slot in range(count):
        block = ids_ref[slot, position] // devices
        loads[slot].wait()
        pltpu.make_async_copy(data.at[slot], out_ref.at[block], store_sem).start()
    pltpu.make_async_copy(data, out_ref, store_sem).wait()


def reduce_groups(place_hbm, *refs):
    tile_refs, (received_ref, share_ref, data, sums, tiles, place_ref, place_sem, load_sems) = refs[:-8], refs[-8:]
    blocks, per_block, rows, width = data.shape
    loads = [
        pltpu.make_async_copy(received_ref.at[pl.ds(b * per_block, per_block)], data.at[b], load_sems.at[b])
        for b in range(blocks)
    ]
    for load in loads:
        load.start()
    place_copy = pltpu.make_async_copy(place_hbm, place_ref, place_sem)
    place_copy.start()
    count = len(tile_refs)
    my_row = lax.axis_index(ROW)
    for step, tile_ref in enumerate(tile_refs):
        tiles[(my_row - step + count) % count] = tile_ref[...]
    factor = jnp.concatenate([tiles[i] for i in range(count)], axis=0)
    rank = factor.shape[0]
    factor_high = factor.astype(jnp.bfloat16)
    factor_low = (factor - factor_high.astype(jnp.float32)).astype(jnp.bfloat16)
    filler = jnp.zeros((128 - 2 * rank, width), jnp.bfloat16)
    factors = jnp.concatenate([factor_high, factor_low, filler], axis=0)
    lane = lax.broadcasted_iota(jnp.int32, (per_block * rows, 128), 1)
    place_copy.wait()
    for b in range(blocks):
        loads[b].wait()
        part = data[b].reshape(per_block * rows, width)
        high = part.astype(jnp.bfloat16)
        low = (part - high.astype(jnp.float32)).astype(jnp.bfloat16)
        over = (((1,), (1,)), ((), ()))
        product = lax.dot_general(high, factors, over, preferred_element_type=jnp.float32)
        product += lax.dot_general(low, factors, over, preferred_element_type=jnp.float32)
        squares = jnp.sum(part * part, axis=1, keepdims=True)
        product = jnp.where(lane == 2 * rank, squares, product)
        for i in range(per_block):
            place = place_ref[b * per_block + i]
            sums[pl.ds(pl.multiple_of(place * rows, rows), rows), :] = product[i * rows : (i + 1) * rows]
    half = rank // 2
    for c in range(0, share_ref.shape[0], 2):
        turned = sums[c * 64 : (c + 2) * 64, :].T
        shares = turned[:rank] + turned[rank : 2 * rank]
        squares = turned[2 * rank : 2 * rank + 8]
        for i in range(2):
            lanes = slice(i * 64, (i + 1) * 64)
            share_ref[c + i, :half, :] = jnp.concatenate([shares[:half, lanes], shares[half:, lanes]], axis=1)
            share_ref[c + i, half:, :] = jnp.concatenate([squares[:, lanes], squares[:, lanes]], axis=1)


def place_groups(place_hbm, received_ref, relaid_ref, data, place_ref, place_sem, load_sems, store_sem):
    blocks, per_block = data.shape[:2]
    place_copy = pltpu.make_async_copy(place_hbm, place_ref, place_sem)
    place_copy.start()
    loads = [
        pltpu.make_async_copy(received_ref.at[pl.ds(b * per_block, per_block)], data.at[b], load_sems.at[b])
        for b in range(blocks)
    ]
    for load in loads:
        load.start()
    place_copy.wait()
    for b in range(blocks):
        loads[b].wait()
        for i in range(per_block):
            place = place_ref[b * per_block + i]
            pltpu.make_async_copy(data.at[b, i], relaid_ref.at[place], store_sem).start()
    pltpu.make_async_copy(received_ref, relaid_ref, store_sem).wait()


def finish(shares_ref, projection_ref, norms_ref, *, full_width):
    half = projection_ref.shape[0] // 2
    total = jnp.sum(shares_ref[...], axis=0)
    projection_ref[:half, :] = total[:half, :64]
    projection_ref[half:, :] = total[:half, 64:]
    norms_ref[...] = jnp.sqrt(total[half : half + 1, :64] / full_width + epsilon)


def on_device(old_residual, group_map, q_factor):
    rows_total = lax.axis_size(ROW)
    columns_total = lax.axis_size(COL)
    devices = rows_total * columns_total
    group_rows = old_residual.shape[0] // rows_total
    full_width = old_residual.shape[1]
    width = full_width // columns_total
    rank = q_factor.shape[1] * rows_total
    own_rows = devices * group_rows // columns_total
    ids = group_map.T
    source = old_residual.reshape(rows_total, group_rows, columns_total, width).transpose(0, 2, 1, 3)
    hbm = pl.BlockSpec(memory_space=pltpu.HBM)
    vmem = pl.BlockSpec(memory_space=pltpu.VMEM)
    f32 = jnp.float32
    dma = pltpu.SemaphoreType.DMA
    pieces = pl.pallas_call(
        order_slots,
        out_shape=jax.ShapeDtypeStruct(source.shape, f32),
        in_specs=[hbm, hbm],
        out_specs=hbm,
        scratch_shapes=[
            pltpu.VMEM(source.shape, f32),
            pltpu.SMEM(ids.shape, jnp.int32),
            dma,
            dma((rows_total,)),
            dma,
        ],
        name="order_slots",
    )(ids, source)
    pieces = pieces.reshape(devices, group_rows, width)
    received = lax.all_to_all(pieces, ALL, 0, 0, tiled=True)
    tiles = [q_factor.T]
    for step in range(1, rows_total):
        ring = [(i, (i + step) % rows_total) for i in range(rows_total)]
        tiles.append(lax.ppermute(tiles[0], ROW, ring))
    place = jnp.sum(jnp.where(ids // devices == lax.axis_index(ROW), ids % devices, 0), axis=0)
    blocks = 4
    staged = (blocks, devices // blocks, group_rows, width)
    shares = pl.pallas_call(
        reduce_groups,
        out_shape=jax.ShapeDtypeStruct((columns_total, rank // 2 + 8, 2 * own_rows), f32),
        in_specs=[hbm] + [vmem] * rows_total + [hbm],
        out_specs=vmem,
        scratch_shapes=[
            pltpu.VMEM(staged, f32),
            pltpu.VMEM((devices * group_rows, 128), f32),
            pltpu.VMEM((rows_total, rank // rows_total, width), f32),
            pltpu.SMEM((devices,), jnp.int32),
            dma,
            dma((blocks,)),
        ],
        compiler_params=pltpu.CompilerParams(vmem_limit_bytes=16 * MIB),
        name="reduce_groups",
    )(place, *tiles, received)
    relaid = pl.pallas_call(
        place_groups,
        out_shape=jax.ShapeDtypeStruct(received.shape, f32),
        in_specs=[hbm, hbm],
        out_specs=hbm,
        scratch_shapes=[
            pltpu.VMEM(staged, f32),
            pltpu.SMEM((devices,), jnp.int32),
            dma,
            dma((blocks,)),
            dma,
        ],
        name="place_groups",
    )(place, received)
    shares = lax.all_to_all(shares, COL, 0, 0, tiled=True)
    projection, norms = pl.pallas_call(
        lambda *refs: finish(*refs, full_width=full_width),
        out_shape=(
            jax.ShapeDtypeStruct((rank, own_rows), f32),
            jax.ShapeDtypeStruct((1, own_rows), f32),
        ),
        in_specs=[vmem],
        out_specs=(vmem, vmem),
        compiler_params=pltpu.CompilerParams(vmem_limit_bytes=4 * MIB),
        name="finish",
    )(shares)
    return relaid.reshape(devices * group_rows, width), projection, norms.reshape(own_rows)


def solution(mesh):
    parts = Mesh(mesh.devices.reshape(4, 2, 4, 2, 2), ALL)
    return jax.shard_map(
        on_device,
        mesh=parts,
        in_specs=(P(ALL, None), P(), P(COL, ROW)),
        out_specs=(P(ROW, COL), P(None, ALL), P(ALL)),
        check_vma=False,
    )
```

```python
import jax
import jax.numpy as jnp
from jax import lax
from jax.experimental import pallas as pl
from jax.experimental.pallas import tpu as pltpu
from jax.sharding import Mesh, PartitionSpec as P

epsilon = 1e-06
ROW = ("x", "yh")
COL = ("z", "yl", "core")
ALL = ROW + COL
EXCHANGE = ("yh", "core", "yl", "z", "x")
MIB = 1 << 20


def order_slots(ids_hbm, source_ref, out_ref, data, ids_ref, ids_sem, load_sems, store_sem):
    slots, _, halves, cores = source_ref.shape[:4]
    devices = ids_hbm.shape[1]
    ids_copy = pltpu.make_async_copy(ids_hbm, ids_ref, ids_sem)
    ids_copy.start()
    loads = [pltpu.make_async_copy(source_ref.at[j], data.at[j], load_sems.at[j]) for j in range(slots)]
    for load in loads:
        load.start()
    position = lax.axis_index(ALL)
    ids_copy.wait()
    for slot in range(slots):
        block = ids_ref[slot, position] // devices
        x, yh = block // out_ref.shape[0], block % out_ref.shape[0]
        loads[slot].wait()
        for yl in range(halves):
            for core in range(cores):
                pltpu.make_async_copy(data.at[slot, :, yl, core], out_ref.at[yh, core, yl, :, x], store_sem).start()
    pltpu.make_async_copy(data, data, store_sem).wait()


def reduce_groups(place_hbm, *refs):
    tile_refs, (received_ref, share_ref, data, sums, tiles, place_ref, place_sem, load_sems) = refs[:-8], refs[-8:]
    blocks, per_block, rows, width = data.shape
    loads = [
        pltpu.make_async_copy(received_ref.at[pl.ds(b * per_block, per_block)], data.at[b], load_sems.at[b])
        for b in range(blocks)
    ]
    for load in loads:
        load.start()
    place_copy = pltpu.make_async_copy(place_hbm, place_ref, place_sem)
    place_copy.start()
    count = len(tile_refs)
    my_row = lax.axis_index(ROW)
    for step, tile_ref in enumerate(tile_refs):
        tiles[(my_row - step + count) % count] = tile_ref[...]
    factor = jnp.concatenate([tiles[i] for i in range(count)], axis=0)
    rank = factor.shape[0]
    factor_high = factor.astype(jnp.bfloat16)
    factor_low = (factor - factor_high.astype(jnp.float32)).astype(jnp.bfloat16)
    filler = jnp.zeros((128 - 2 * rank, width), jnp.bfloat16)
    factors = jnp.concatenate([factor_high, factor_low, filler], axis=0)
    lane = lax.broadcasted_iota(jnp.int32, (per_block * rows, 128), 1)
    place_copy.wait()
    for b in range(blocks):
        loads[b].wait()
        part = data[b].reshape(per_block * rows, width)
        high = part.astype(jnp.bfloat16)
        low = (part - high.astype(jnp.float32)).astype(jnp.bfloat16)
        over = (((1,), (1,)), ((), ()))
        product = lax.dot_general(high, factors, over, preferred_element_type=jnp.float32)
        product += lax.dot_general(low, factors, over, preferred_element_type=jnp.float32)
        squares = jnp.sum(part * part, axis=1, keepdims=True)
        product = jnp.where(lane == 2 * rank, squares, product)
        for i in range(per_block):
            place = place_ref[b * per_block + i]
            sums[pl.ds(pl.multiple_of(place * rows, rows), rows), :] = product[i * rows : (i + 1) * rows]
    half = rank // 2
    for c in range(0, share_ref.shape[0], 2):
        turned = sums[c * 64 : (c + 2) * 64, :].T
        shares = turned[:rank] + turned[rank : 2 * rank]
        squares = turned[2 * rank : 2 * rank + 8]
        for i in range(2):
            lanes = slice(i * 64, (i + 1) * 64)
            share_ref[c + i, :half, :] = jnp.concatenate([shares[:half, lanes], shares[half:, lanes]], axis=1)
            share_ref[c + i, half:, :] = jnp.concatenate([squares[:, lanes], squares[:, lanes]], axis=1)


def place_groups(place_hbm, received_ref, relaid_ref, data, place_ref, place_sem, load_sems, store_sem):
    blocks, per_block = data.shape[:2]
    place_copy = pltpu.make_async_copy(place_hbm, place_ref, place_sem)
    place_copy.start()
    loads = [
        pltpu.make_async_copy(received_ref.at[pl.ds(b * per_block, per_block)], data.at[b], load_sems.at[b])
        for b in range(blocks)
    ]
    for load in loads:
        load.start()
    place_copy.wait()
    for b in range(blocks):
        loads[b].wait()
        for i in range(per_block):
            place = place_ref[b * per_block + i]
            pltpu.make_async_copy(data.at[b, i], relaid_ref.at[place], store_sem).start()
    pltpu.make_async_copy(received_ref, relaid_ref, store_sem).wait()


def finish(shares_ref, projection_ref, norms_ref, *, full_width):
    half = projection_ref.shape[0] // 2
    total = jnp.sum(shares_ref[...], axis=0)
    projection_ref[:half, :] = total[:half, :64]
    projection_ref[half:, :] = total[:half, 64:]
    norms_ref[...] = jnp.sqrt(total[half : half + 1, :64] / full_width + epsilon)


def on_device(old_residual, group_map, q_factor):
    rows_total = lax.axis_size(ROW)
    columns_total = lax.axis_size(COL)
    devices = rows_total * columns_total
    group_rows = old_residual.shape[0] // rows_total
    full_width = old_residual.shape[1]
    width = full_width // columns_total
    rank = q_factor.shape[1] * rows_total
    own_rows = devices * group_rows // columns_total
    ids = group_map.T
    sizes = {name: lax.axis_size(name) for name in ALL}
    by_column = [sizes[name] for name in COL]
    source = old_residual.reshape(rows_total, group_rows, *by_column, width).transpose(0, 2, 3, 4, 1, 5)
    ordered = tuple(sizes[name] for name in EXCHANGE) + (group_rows, width)
    hbm = pl.BlockSpec(memory_space=pltpu.HBM)
    vmem = pl.BlockSpec(memory_space=pltpu.VMEM)
    f32 = jnp.float32
    dma = pltpu.SemaphoreType.DMA
    pieces = pl.pallas_call(
        order_slots,
        out_shape=jax.ShapeDtypeStruct(ordered, f32),
        in_specs=[hbm, hbm],
        out_specs=hbm,
        scratch_shapes=[
            pltpu.VMEM(source.shape, f32),
            pltpu.SMEM(ids.shape, jnp.int32),
            dma,
            dma((rows_total,)),
            dma,
        ],
        name="order_slots",
    )(ids, source)
    pieces = pieces.reshape(devices, group_rows, width)
    received = lax.all_to_all(pieces, EXCHANGE, 0, 0, tiled=True)
    tiles = [q_factor.T]
    for step in range(1, rows_total):
        ring = [(i, (i + step) % rows_total) for i in range(rows_total)]
        tiles.append(lax.ppermute(tiles[0], ROW, ring))
    place = jnp.sum(jnp.where(ids // devices == lax.axis_index(ROW), ids % devices, 0), axis=0)
    place = place.reshape([sizes[name] for name in ALL]).transpose([ALL.index(name) for name in EXCHANGE])
    place = place.reshape(devices)
    blocks = 4
    staged = (blocks, devices // blocks, group_rows, width)
    shares = pl.pallas_call(
        reduce_groups,
        out_shape=jax.ShapeDtypeStruct((columns_total, rank // 2 + 8, 2 * own_rows), f32),
        in_specs=[hbm] + [vmem] * rows_total + [hbm],
        out_specs=vmem,
        scratch_shapes=[
            pltpu.VMEM(staged, f32),
            pltpu.VMEM((devices * group_rows, 128), f32),
            pltpu.VMEM((rows_total, rank // rows_total, width), f32),
            pltpu.SMEM((devices,), jnp.int32),
            dma,
            dma((blocks,)),
        ],
        compiler_params=pltpu.CompilerParams(vmem_limit_bytes=16 * MIB),
        name="reduce_groups",
    )(place, *tiles, received)
    relaid = pl.pallas_call(
        place_groups,
        out_shape=jax.ShapeDtypeStruct(received.shape, f32),
        in_specs=[hbm, hbm],
        out_specs=hbm,
        scratch_shapes=[
            pltpu.VMEM(staged, f32),
            pltpu.SMEM((devices,), jnp.int32),
            dma,
            dma((blocks,)),
            dma,
        ],
        name="place_groups",
    )(place, received)
    shares = lax.all_to_all(shares, COL, 0, 0, tiled=True)
    projection, norms = pl.pallas_call(
        lambda *refs: finish(*refs, full_width=full_width),
        out_shape=(
            jax.ShapeDtypeStruct((rank, own_rows), f32),
            jax.ShapeDtypeStruct((1, own_rows), f32),
        ),
        in_specs=[vmem],
        out_specs=(vmem, vmem),
        compiler_params=pltpu.CompilerParams(vmem_limit_bytes=4 * MIB),
        name="finish",
    )(shares)
    return relaid.reshape(devices * group_rows, width), projection, norms.reshape(own_rows)


def solution(mesh):
    parts = Mesh(mesh.devices.reshape(4, 2, 4, 2, 2), ALL)
    return jax.shard_map(
        on_device,
        mesh=parts,
        in_specs=(P(ALL, None), P(), P(COL, ROW)),
        out_specs=(P(ROW, COL), P(None, ALL), P(ALL)),
        check_vma=False,
    )
```

```python
import jax
import jax.numpy as jnp
from jax import lax
from jax.experimental import pallas as pl
from jax.experimental.pallas import tpu as pltpu
from jax.sharding import Mesh, PartitionSpec as P

epsilon = 1e-06
ROW = ("x", "yh")
COL = ("z", "yl", "core")
ALL = ROW + COL
EXCHANGE = ("yh", "core", "yl", "z", "x")
MIB = 1 << 20


def order_slots(ids_hbm, source_ref, out_ref, data, ids_ref, ids_sem, load_sems, store_sem):
    slots, _, halves, cores = source_ref.shape[:4]
    devices = ids_hbm.shape[1]
    ids_copy = pltpu.make_async_copy(ids_hbm, ids_ref, ids_sem)
    ids_copy.start()
    loads = [pltpu.make_async_copy(source_ref.at[j], data.at[j], load_sems.at[j]) for j in range(slots)]
    for load in loads:
        load.start()
    position = lax.axis_index(ALL)
    ids_copy.wait()
    for slot in range(slots):
        block = ids_ref[slot, position] // devices
        x, yh = block // out_ref.shape[0], block % out_ref.shape[0]
        loads[slot].wait()
        for yl in range(halves):
            for core in range(cores):
                pltpu.make_async_copy(data.at[slot, :, yl, core], out_ref.at[yh, core, yl, :, x], store_sem).start()
    pltpu.make_async_copy(data, data, store_sem).wait()


def reduce_groups(place_hbm, *refs):
    tile_refs, (received_ref, share_ref, data, sums, tiles, place_ref, place_sem, load_sems) = refs[:-8], refs[-8:]
    blocks, per_block, rows, width = data.shape
    loads = [
        pltpu.make_async_copy(received_ref.at[pl.ds(b * per_block, per_block)], data.at[b], load_sems.at[b])
        for b in range(blocks)
    ]
    for load in loads:
        load.start()
    place_copy = pltpu.make_async_copy(place_hbm, place_ref, place_sem)
    place_copy.start()
    count = len(tile_refs)
    my_row = lax.axis_index(ROW)
    for step, tile_ref in enumerate(tile_refs):
        tiles[(my_row - step + count) % count] = tile_ref[...]
    factor = jnp.concatenate([tiles[i] for i in range(count)], axis=0)
    rank = factor.shape[0]
    factor_high = factor.astype(jnp.bfloat16)
    factor_low = (factor - factor_high.astype(jnp.float32)).astype(jnp.bfloat16)
    filler = jnp.zeros((128 - 2 * rank, width), jnp.bfloat16)
    factors = jnp.concatenate([factor_high, factor_low, filler], axis=0)
    lane = lax.broadcasted_iota(jnp.int32, (per_block * rows, 128), 1)
    place_copy.wait()
    def block(b, carry):
        pltpu.make_async_copy(received_ref.at[pl.ds(b * per_block, per_block)], data.at[b], load_sems.at[b]).wait()
        part = data[b].reshape(per_block * rows, width)
        high = part.astype(jnp.bfloat16)
        low = (part - high.astype(jnp.float32)).astype(jnp.bfloat16)
        over = (((1,), (1,)), ((), ()))
        product = lax.dot_general(high, factors, over, preferred_element_type=jnp.float32)
        product += lax.dot_general(low, factors, over, preferred_element_type=jnp.float32)
        squares = jnp.sum(part * part, axis=1, keepdims=True)
        product = jnp.where(lane == 2 * rank, squares, product)
        for i in range(per_block):
            place = place_ref[b * per_block + i]
            sums[pl.ds(pl.multiple_of(place * rows, rows), rows), :] = product[i * rows : (i + 1) * rows]
        return carry

    lax.fori_loop(0, blocks, block, 0)
    half = rank // 2
    for c in range(0, share_ref.shape[0], 2):
        turned = sums[c * 64 : (c + 2) * 64, :].T
        shares = turned[:rank] + turned[rank : 2 * rank]
        squares = turned[2 * rank : 2 * rank + 8]
        for i in range(2):
            lanes = slice(i * 64, (i + 1) * 64)
            packed = jnp.concatenate([shares[:half, lanes], shares[half:, lanes]], axis=1)
            for k in range(half):
                share_ref[c + i, :, k * 128 : (k + 1) * 128] = packed[k : k + 1]
            spread = jnp.concatenate([squares[:1, lanes], squares[:1, lanes]], axis=1)
            share_ref[c + i, :, half * 128 : (half + 1) * 128] = spread


def place_groups(place_hbm, received_ref, relaid_ref, data, place_ref, place_sem, load_sems, store_sem):
    blocks, per_block = data.shape[:2]
    place_copy = pltpu.make_async_copy(place_hbm, place_ref, place_sem)
    place_copy.start()
    loads = [
        pltpu.make_async_copy(received_ref.at[pl.ds(b * per_block, per_block)], data.at[b], load_sems.at[b])
        for b in range(blocks)
    ]
    for load in loads:
        load.start()
    place_copy.wait()
    for b in range(blocks):
        loads[b].wait()
        for i in range(per_block):
            place = place_ref[b * per_block + i]
            pltpu.make_async_copy(data.at[b, i], relaid_ref.at[place], store_sem).start()
    pltpu.make_async_copy(received_ref, relaid_ref, store_sem).wait()


def finish(shares_ref, projection_ref, norms_ref, *, full_width):
    half = projection_ref.shape[0] // 2
    total = jnp.sum(shares_ref[...], axis=0)
    for k in range(half):
        projection_ref[k : k + 1, :] = total[:, k * 128 : k * 128 + 64]
        projection_ref[half + k : half + k + 1, :] = total[:, k * 128 + 64 : (k + 1) * 128]
    norms_ref[...] = jnp.sqrt(total[:, half * 128 : half * 128 + 64] / full_width + epsilon)


def on_device(old_residual, group_map, q_factor):
    rows_total = lax.axis_size(ROW)
    columns_total = lax.axis_size(COL)
    devices = rows_total * columns_total
    group_rows = old_residual.shape[0] // rows_total
    full_width = old_residual.shape[1]
    width = full_width // columns_total
    rank = q_factor.shape[1] * rows_total
    own_rows = devices * group_rows // columns_total
    ids = group_map.T
    sizes = {name: lax.axis_size(name) for name in ALL}
    by_column = [sizes[name] for name in COL]
    source = old_residual.reshape(rows_total, group_rows, *by_column, width).transpose(0, 2, 3, 4, 1, 5)
    ordered = tuple(sizes[name] for name in EXCHANGE) + (group_rows, width)
    hbm = pl.BlockSpec(memory_space=pltpu.HBM)
    vmem = pl.BlockSpec(memory_space=pltpu.VMEM)
    f32 = jnp.float32
    dma = pltpu.SemaphoreType.DMA
    pieces = pl.pallas_call(
        order_slots,
        out_shape=jax.ShapeDtypeStruct(ordered, f32),
        in_specs=[hbm, hbm],
        out_specs=hbm,
        scratch_shapes=[
            pltpu.VMEM(source.shape, f32),
            pltpu.SMEM(ids.shape, jnp.int32),
            dma,
            dma((rows_total,)),
            dma,
        ],
        name="order_slots",
    )(ids, source)
    pieces = pieces.reshape(devices, group_rows, width)
    received = lax.all_to_all(pieces, EXCHANGE, 0, 0, tiled=True)
    tiles = [q_factor.T]
    for step in range(1, rows_total):
        ring = [(i, (i + step) % rows_total) for i in range(rows_total)]
        tiles.append(lax.ppermute(tiles[0], ROW, ring))
    place = jnp.sum(jnp.where(ids // devices == lax.axis_index(ROW), ids % devices, 0), axis=0)
    place = place.reshape([sizes[name] for name in ALL]).transpose([ALL.index(name) for name in EXCHANGE])
    place = place.reshape(devices)
    blocks = 4
    staged = (blocks, devices // blocks, group_rows, width)
    shares = pl.pallas_call(
        reduce_groups,
        out_shape=jax.ShapeDtypeStruct((columns_total, 1, (rank // 2 + 1) * 2 * own_rows), f32),
        in_specs=[hbm] + [vmem] * rows_total + [hbm],
        out_specs=vmem,
        scratch_shapes=[
            pltpu.VMEM(staged, f32),
            pltpu.VMEM((devices * group_rows, 128), f32),
            pltpu.VMEM((rows_total, rank // rows_total, width), f32),
            pltpu.SMEM((devices,), jnp.int32),
            dma,
            dma((blocks,)),
        ],
        compiler_params=pltpu.CompilerParams(vmem_limit_bytes=16 * MIB),
        name="reduce_groups",
    )(place, *tiles, received)
    relaid = pl.pallas_call(
        place_groups,
        out_shape=jax.ShapeDtypeStruct(received.shape, f32),
        in_specs=[hbm, hbm],
        out_specs=hbm,
        scratch_shapes=[
            pltpu.VMEM(staged, f32),
            pltpu.SMEM((devices,), jnp.int32),
            dma,
            dma((blocks,)),
            dma,
        ],
        name="place_groups",
    )(place, received)
    shares = lax.all_to_all(shares, COL, 0, 0, tiled=True)
    projection, norms = pl.pallas_call(
        lambda *refs: finish(*refs, full_width=full_width),
        out_shape=(
            jax.ShapeDtypeStruct((rank, own_rows), f32),
            jax.ShapeDtypeStruct((1, own_rows), f32),
        ),
        in_specs=[vmem],
        out_specs=(vmem, vmem),
        compiler_params=pltpu.CompilerParams(vmem_limit_bytes=4 * MIB),
        name="finish",
    )(shares)
    return relaid.reshape(devices * group_rows, width), projection, norms.reshape(own_rows)


def solution(mesh):
    parts = Mesh(mesh.devices.reshape(4, 2, 4, 2, 2), ALL)
    return jax.shard_map(
        on_device,
        mesh=parts,
        in_specs=(P(ALL, None), P(), P(COL, ROW)),
        out_specs=(P(ROW, COL), P(None, ALL), P(ALL)),
        check_vma=False,
    )
```

```python
import jax
import jax.numpy as jnp
from jax import lax
from jax.experimental import pallas as pl
from jax.experimental.pallas import tpu as pltpu
from jax.sharding import Mesh, PartitionSpec as P

epsilon = 1e-06
ROW = ("x", "yh")
COL = ("z", "yl", "core")
ALL = ROW + COL
EXCHANGE = ("yh", "core", "yl", "z", "x")
MIB = 1 << 20


def order_slots(ids_hbm, source_ref, out_ref, data, ids_ref, ids_sem, load_sems, store_sem):
    slots, _, halves, cores = source_ref.shape[:4]
    devices = ids_hbm.shape[1]
    ids_copy = pltpu.make_async_copy(ids_hbm, ids_ref, ids_sem)
    ids_copy.start()
    loads = [pltpu.make_async_copy(source_ref.at[j], data.at[j], load_sems.at[j]) for j in range(slots)]
    for load in loads:
        load.start()
    position = lax.axis_index(ALL)
    ids_copy.wait()
    for slot in range(slots):
        block = ids_ref[slot, position] // devices
        x, yh = block // out_ref.shape[0], block % out_ref.shape[0]
        loads[slot].wait()
        for yl in range(halves):
            for core in range(cores):
                pltpu.make_async_copy(data.at[slot, :, yl, core], out_ref.at[yh, core, yl, :, x], store_sem).start()
    pltpu.make_async_copy(data, data, store_sem).wait()


def reduce_groups(place_hbm, *refs):
    tile_refs, refs = refs[:-10], refs[-10:]
    received_ref, relaid_ref, share_ref, data, sums, tiles, place_ref, place_sem, load_sems, store_sem = refs
    blocks, per_block, rows, width = data.shape
    loads = [
        pltpu.make_async_copy(received_ref.at[pl.ds(b * per_block, per_block)], data.at[b], load_sems.at[b])
        for b in range(blocks)
    ]
    for load in loads:
        load.start()
    place_copy = pltpu.make_async_copy(place_hbm, place_ref, place_sem)
    place_copy.start()
    count = len(tile_refs)
    my_row = lax.axis_index(ROW)
    for step, tile_ref in enumerate(tile_refs):
        tiles[(my_row - step + count) % count] = tile_ref[...]
    factor = jnp.concatenate([tiles[i] for i in range(count)], axis=0)
    rank = factor.shape[0]
    factor_high = factor.astype(jnp.bfloat16)
    factor_low = (factor - factor_high.astype(jnp.float32)).astype(jnp.bfloat16)
    filler = jnp.zeros((128 - 2 * rank, width), jnp.bfloat16)
    factors = jnp.concatenate([factor_high, factor_low, filler], axis=0)
    lane = lax.broadcasted_iota(jnp.int32, (per_block * rows, 128), 1)
    place_copy.wait()
    def block(b, carry):
        pltpu.make_async_copy(received_ref.at[pl.ds(b * per_block, per_block)], data.at[b], load_sems.at[b]).wait()
        for i in range(per_block):
            place = place_ref[b * per_block + i]
            pltpu.make_async_copy(data.at[b, i], relaid_ref.at[place], store_sem).start()
        part = data[b].reshape(per_block * rows, width)
        high = part.astype(jnp.bfloat16)
        low = (part - high.astype(jnp.float32)).astype(jnp.bfloat16)
        over = (((1,), (1,)), ((), ()))
        product = lax.dot_general(high, factors, over, preferred_element_type=jnp.float32)
        product += lax.dot_general(low, factors, over, preferred_element_type=jnp.float32)
        squares = jnp.sum(part * part, axis=1, keepdims=True)
        product = jnp.where(lane == 2 * rank, squares, product)
        for i in range(per_block):
            place = place_ref[b * per_block + i]
            sums[pl.ds(pl.multiple_of(place * rows, rows), rows), :] = product[i * rows : (i + 1) * rows]
        return carry

    lax.fori_loop(0, blocks, block, 0)
    half = rank // 2
    for c in range(0, share_ref.shape[0], 2):
        turned = sums[c * 64 : (c + 2) * 64, :].T
        shares = turned[:rank] + turned[rank : 2 * rank]
        squares = turned[2 * rank : 2 * rank + 8]
        for i in range(2):
            lanes = slice(i * 64, (i + 1) * 64)
            packed = jnp.concatenate([shares[:half, lanes], shares[half:, lanes]], axis=1)
            for k in range(half):
                share_ref[c + i, :, k * 128 : (k + 1) * 128] = packed[k : k + 1]
            spread = jnp.concatenate([squares[:1, lanes], squares[:1, lanes]], axis=1)
            share_ref[c + i, :, half * 128 : (half + 1) * 128] = spread
    pltpu.make_async_copy(received_ref, relaid_ref, store_sem).wait()


def finish(shares_ref, projection_ref, norms_ref, *, full_width):
    half = projection_ref.shape[0] // 2
    total = jnp.sum(shares_ref[...], axis=0)
    for k in range(half):
        projection_ref[k : k + 1, :] = total[:, k * 128 : k * 128 + 64]
        projection_ref[half + k : half + k + 1, :] = total[:, k * 128 + 64 : (k + 1) * 128]
    norms_ref[...] = jnp.sqrt(total[:, half * 128 : half * 128 + 64] / full_width + epsilon)


def on_device(old_residual, group_map, q_factor):
    rows_total = lax.axis_size(ROW)
    columns_total = lax.axis_size(COL)
    devices = rows_total * columns_total
    group_rows = old_residual.shape[0] // rows_total
    full_width = old_residual.shape[1]
    width = full_width // columns_total
    rank = q_factor.shape[1] * rows_total
    own_rows = devices * group_rows // columns_total
    ids = group_map.T
    sizes = {name: lax.axis_size(name) for name in ALL}
    by_column = [sizes[name] for name in COL]
    source = old_residual.reshape(rows_total, group_rows, *by_column, width).transpose(0, 2, 3, 4, 1, 5)
    ordered = tuple(sizes[name] for name in EXCHANGE) + (group_rows, width)
    hbm = pl.BlockSpec(memory_space=pltpu.HBM)
    vmem = pl.BlockSpec(memory_space=pltpu.VMEM)
    f32 = jnp.float32
    dma = pltpu.SemaphoreType.DMA
    pieces = pl.pallas_call(
        order_slots,
        out_shape=jax.ShapeDtypeStruct(ordered, f32),
        in_specs=[hbm, hbm],
        out_specs=hbm,
        scratch_shapes=[
            pltpu.VMEM(source.shape, f32),
            pltpu.SMEM(ids.shape, jnp.int32),
            dma,
            dma((rows_total,)),
            dma,
        ],
        name="order_slots",
    )(ids, source)
    pieces = pieces.reshape(devices, group_rows, width)
    received = lax.all_to_all(pieces, EXCHANGE, 0, 0, tiled=True)
    tiles = [q_factor.T]
    for step in range(1, rows_total):
        ring = [(i, (i + step) % rows_total) for i in range(rows_total)]
        tiles.append(lax.ppermute(tiles[0], ROW, ring))
    place = jnp.sum(jnp.where(ids // devices == lax.axis_index(ROW), ids % devices, 0), axis=0)
    place = place.reshape([sizes[name] for name in ALL]).transpose([ALL.index(name) for name in EXCHANGE])
    place = place.reshape(devices)
    blocks = 4
    staged = (blocks, devices // blocks, group_rows, width)
    relaid, shares = pl.pallas_call(
        reduce_groups,
        out_shape=(
            jax.ShapeDtypeStruct(received.shape, f32),
            jax.ShapeDtypeStruct((columns_total, 1, (rank // 2 + 1) * 2 * own_rows), f32),
        ),
        in_specs=[hbm] + [vmem] * rows_total + [hbm],
        out_specs=(hbm, vmem),
        scratch_shapes=[
            pltpu.VMEM(staged, f32),
            pltpu.VMEM((devices * group_rows, 128), f32),
            pltpu.VMEM((rows_total, rank // rows_total, width), f32),
            pltpu.SMEM((devices,), jnp.int32),
            dma,
            dma((blocks,)),
            dma,
        ],
        compiler_params=pltpu.CompilerParams(vmem_limit_bytes=16 * MIB),
        name="reduce_groups",
    )(place, *tiles, received)
    shares = lax.all_to_all(shares, COL, 0, 0, tiled=True)
    projection, norms = pl.pallas_call(
        lambda *refs: finish(*refs, full_width=full_width),
        out_shape=(
            jax.ShapeDtypeStruct((rank, own_rows), f32),
            jax.ShapeDtypeStruct((1, own_rows), f32),
        ),
        in_specs=[vmem],
        out_specs=(vmem, vmem),
        compiler_params=pltpu.CompilerParams(vmem_limit_bytes=4 * MIB),
        name="finish",
    )(shares)
    return relaid.reshape(devices * group_rows, width), projection, norms.reshape(own_rows)


def solution(mesh):
    parts = Mesh(mesh.devices.reshape(4, 2, 4, 2, 2), ALL)
    return jax.shard_map(
        on_device,
        mesh=parts,
        in_specs=(P(ALL, None), P(), P(COL, ROW)),
        out_specs=(P(ROW, COL), P(None, ALL), P(ALL)),
        check_vma=False,
    )
```

```python
import jax
import jax.numpy as jnp
from jax import lax
from jax.experimental import pallas as pl
from jax.experimental.pallas import tpu as pltpu
from jax.sharding import Mesh, PartitionSpec as P

epsilon = 1e-06
ROW = ("x", "yh")
COL = ("z", "yl", "core")
ALL = ROW + COL
EXCHANGE = ('z', 'core', 'x', 'yl', 'yh')
MIB = 1 << 20


def order_slots(ids_hbm, source_ref, out_ref, data, ids_ref, ids_sem, load_sems, store_sem):
    slots, _, halves, cores = source_ref.shape[:4]
    devices = ids_hbm.shape[1]
    ids_copy = pltpu.make_async_copy(ids_hbm, ids_ref, ids_sem)
    ids_copy.start()
    loads = [pltpu.make_async_copy(source_ref.at[j], data.at[j], load_sems.at[j]) for j in range(slots)]
    for load in loads:
        load.start()
    position = lax.axis_index(ALL)
    ids_copy.wait()
    for slot in range(slots):
        block = ids_ref[slot, position] // devices
        x, yh = block // 2, block % 2
        loads[slot].wait()
        for yl in range(halves):
            for core in range(cores):
                at = {"x": x, "yh": yh, "yl": yl, "core": core, "z": slice(None)}
                piece = out_ref.at[tuple(at[name] for name in EXCHANGE)]
                pltpu.make_async_copy(data.at[slot, :, yl, core], piece, store_sem).start()
    pltpu.make_async_copy(data, data, store_sem).wait()


def reduce_groups(place_hbm, *refs):
    tile_refs, refs = refs[:-10], refs[-10:]
    received_ref, relaid_ref, share_ref, data, sums, tiles, place_ref, place_sem, load_sems, store_sem = refs
    blocks, per_block, rows, width = data.shape
    loads = [
        pltpu.make_async_copy(received_ref.at[pl.ds(b * per_block, per_block)], data.at[b], load_sems.at[b])
        for b in range(blocks)
    ]
    for load in loads:
        load.start()
    place_copy = pltpu.make_async_copy(place_hbm, place_ref, place_sem)
    place_copy.start()
    count = len(tile_refs)
    my_row = lax.axis_index(ROW)
    for step, tile_ref in enumerate(tile_refs):
        tiles[(my_row - step + count) % count] = tile_ref[...]
    factor = jnp.concatenate([tiles[i] for i in range(count)], axis=0)
    rank = factor.shape[0]
    factor_high = factor.astype(jnp.bfloat16)
    factor_low = (factor - factor_high.astype(jnp.float32)).astype(jnp.bfloat16)
    filler = jnp.zeros((128 - 2 * rank, width), jnp.bfloat16)
    factors = jnp.concatenate([factor_high, factor_low, filler], axis=0)
    lane = lax.broadcasted_iota(jnp.int32, (per_block * rows, 128), 1)
    place_copy.wait()
    def block(b, carry):
        pltpu.make_async_copy(received_ref.at[pl.ds(b * per_block, per_block)], data.at[b], load_sems.at[b]).wait()
        for i in range(per_block):
            place = place_ref[b * per_block + i]
            pltpu.make_async_copy(data.at[b, i], relaid_ref.at[place], store_sem).start()
        part = data[b].reshape(per_block * rows, width)
        high = part.astype(jnp.bfloat16)
        low = (part - high.astype(jnp.float32)).astype(jnp.bfloat16)
        over = (((1,), (1,)), ((), ()))
        product = lax.dot_general(high, factors, over, preferred_element_type=jnp.float32)
        product += lax.dot_general(low, factors, over, preferred_element_type=jnp.float32)
        squares = jnp.sum(part * part, axis=1, keepdims=True)
        product = jnp.where(lane == 2 * rank, squares, product)
        for i in range(per_block):
            place = place_ref[b * per_block + i]
            sums[pl.ds(pl.multiple_of(place * rows, rows), rows), :] = product[i * rows : (i + 1) * rows]
        return carry

    lax.fori_loop(0, blocks, block, 0)
    half = rank // 2
    for c in range(0, share_ref.shape[0], 2):
        turned = sums[c * 64 : (c + 2) * 64, :].T
        shares = turned[:rank] + turned[rank : 2 * rank]
        squares = turned[2 * rank : 2 * rank + 8]
        for i in range(2):
            lanes = slice(i * 64, (i + 1) * 64)
            packed = jnp.concatenate([shares[:half, lanes], shares[half:, lanes]], axis=1)
            for k in range(half):
                share_ref[c + i, :, k * 128 : (k + 1) * 128] = packed[k : k + 1]
            spread = jnp.concatenate([squares[:1, lanes], squares[:1, lanes]], axis=1)
            share_ref[c + i, :, half * 128 : (half + 1) * 128] = spread
    pltpu.make_async_copy(received_ref, relaid_ref, store_sem).wait()


def finish(shares_ref, projection_ref, norms_ref, *, full_width):
    half = projection_ref.shape[0] // 2
    total = jnp.sum(shares_ref[...], axis=0)
    for k in range(half):
        projection_ref[k : k + 1, :] = total[:, k * 128 : k * 128 + 64]
        projection_ref[half + k : half + k + 1, :] = total[:, k * 128 + 64 : (k + 1) * 128]
    norms_ref[...] = jnp.sqrt(total[:, half * 128 : half * 128 + 64] / full_width + epsilon)


def on_device(old_residual, group_map, q_factor):
    rows_total = lax.axis_size(ROW)
    columns_total = lax.axis_size(COL)
    devices = rows_total * columns_total
    group_rows = old_residual.shape[0] // rows_total
    full_width = old_residual.shape[1]
    width = full_width // columns_total
    rank = q_factor.shape[1] * rows_total
    own_rows = devices * group_rows // columns_total
    ids = group_map.T
    sizes = {name: lax.axis_size(name) for name in ALL}
    by_column = [sizes[name] for name in COL]
    source = old_residual.reshape(rows_total, group_rows, *by_column, width).transpose(0, 2, 3, 4, 1, 5)
    ordered = tuple(sizes[name] for name in EXCHANGE) + (group_rows, width)
    hbm = pl.BlockSpec(memory_space=pltpu.HBM)
    vmem = pl.BlockSpec(memory_space=pltpu.VMEM)
    f32 = jnp.float32
    dma = pltpu.SemaphoreType.DMA
    pieces = pl.pallas_call(
        order_slots,
        out_shape=jax.ShapeDtypeStruct(ordered, f32),
        in_specs=[hbm, hbm],
        out_specs=hbm,
        scratch_shapes=[
            pltpu.VMEM(source.shape, f32),
            pltpu.SMEM(ids.shape, jnp.int32),
            dma,
            dma((rows_total,)),
            dma,
        ],
        name="order_slots",
    )(ids, source)
    pieces = pieces.reshape(devices, group_rows, width)
    received = lax.all_to_all(pieces, EXCHANGE, 0, 0, tiled=True)
    tiles = [q_factor.T]
    for step in range(1, rows_total):
        ring = [(i, (i + step) % rows_total) for i in range(rows_total)]
        tiles.append(lax.ppermute(tiles[0], ROW, ring))
    place = jnp.sum(jnp.where(ids // devices == lax.axis_index(ROW), ids % devices, 0), axis=0)
    place = place.reshape([sizes[name] for name in ALL]).transpose([ALL.index(name) for name in EXCHANGE])
    place = place.reshape(devices)
    blocks = 4
    staged = (blocks, devices // blocks, group_rows, width)
    relaid, shares = pl.pallas_call(
        reduce_groups,
        out_shape=(
            jax.ShapeDtypeStruct(received.shape, f32),
            jax.ShapeDtypeStruct((columns_total, 1, (rank // 2 + 1) * 2 * own_rows), f32),
        ),
        in_specs=[hbm] + [vmem] * rows_total + [hbm],
        out_specs=(hbm, vmem),
        scratch_shapes=[
            pltpu.VMEM(staged, f32),
            pltpu.VMEM((devices * group_rows, 128), f32),
            pltpu.VMEM((rows_total, rank // rows_total, width), f32),
            pltpu.SMEM((devices,), jnp.int32),
            dma,
            dma((blocks,)),
            dma,
        ],
        compiler_params=pltpu.CompilerParams(vmem_limit_bytes=16 * MIB),
        name="reduce_groups",
    )(place, *tiles, received)
    shares = lax.all_to_all(shares, COL, 0, 0, tiled=True)
    projection, norms = pl.pallas_call(
        lambda *refs: finish(*refs, full_width=full_width),
        out_shape=(
            jax.ShapeDtypeStruct((rank, own_rows), f32),
            jax.ShapeDtypeStruct((1, own_rows), f32),
        ),
        in_specs=[vmem],
        out_specs=(vmem, vmem),
        compiler_params=pltpu.CompilerParams(vmem_limit_bytes=4 * MIB),
        name="finish",
    )(shares)
    return relaid.reshape(devices * group_rows, width), projection, norms.reshape(own_rows)


def solution(mesh):
    parts = Mesh(mesh.devices.reshape(4, 2, 4, 2, 2), ALL)
    return jax.shard_map(
        on_device,
        mesh=parts,
        in_specs=(P(ALL, None), P(), P(COL, ROW)),
        out_specs=(P(ROW, COL), P(None, ALL), P(ALL)),
        check_vma=False,
    )
```
